128 devices in a mesh: dp: 1, ep: 128 (over z, y, x, core).
Axes of the slice: x: 4, y: 4, z: 4, core: 2. Of those that a mesh axis runs over, the one named last changes fastest.
Arguments:
- x_in: bfloat16 [32768, 2048], P(('dp', 'ep'))
- expert_ids: int32 [32768, 8], P(('dp', 'ep'))
- norm_weight: bfloat16 [2048], replicated
- router_w: bfloat16 [2048, 128], replicated
- router_b: bfloat16 [128], replicated
- w_gate_up: bfloat16 [128, 2048, 1536], P('ep')
- b_gate_up: bfloat16 [128, 1536], P('ep')
- w_down: bfloat16 [128, 768, 2048], P('ep')
- b_down: bfloat16 [128, 2048], P('ep')
Outputs:
- output: bfloat16 [32768, 2048], P(('dp', 'ep'))
All inputs are finite; a program needn't handle non-finite values.
Results may differ from the reference program's by a relative error of at most 0.00638535.
Values are sent between devices in bfloat16 or wider.
A program may use at most 1 GiB of HBM per device.

```python
import jax
import jax.numpy as jnp
from jax import lax

D_MODEL = 2048
D_FF = 768
EXPERTS = 128
TOP_K = 8
TOK_DEV = 256
GROUP_SIZE = 128

TOKENS = TOK_DEV * GROUP_SIZE
CAPACITY = 4 * TOP_K * TOK_DEV // EXPERTS
HOT_COUNT = EXPERTS // 8
EPSILON = 1e-5
LIMIT = 7.0
ALPHA = 1.702


def draw_routes(key):
    key_hot, key_src = jax.random.split(key)
    expert_order = jax.random.permutation(key_hot, EXPERTS)
    cold_total = TOP_K * TOK_DEV - HOT_COUNT * CAPACITY
    cold_count = EXPERTS - HOT_COUNT
    position = jnp.arange(EXPERTS)
    extra = (position - HOT_COUNT < cold_total % cold_count).astype(jnp.int32)
    counts = jnp.where(position < HOT_COUNT, CAPACITY, cold_total // cold_count + extra)
    ends = jnp.cumsum(counts)
    slot_rank = jnp.sum(jnp.arange(TOP_K * TOK_DEV)[:, None] >= ends[None, :], axis=1)

    def one_source(src_key):
        key_cold, key_tok = jax.random.split(src_key)
        cold = jax.random.permutation(key_cold, expert_order[HOT_COUNT:])
        order = jnp.concatenate([expert_order[:HOT_COUNT], cold])
        table = order[slot_rank].reshape(TOP_K, TOK_DEV).T
        return table[jax.random.permutation(key_tok, TOK_DEV)]

    tables = jax.vmap(one_source)(jax.random.split(key_src, GROUP_SIZE))
    return tables.reshape(TOKENS, TOP_K).astype(jnp.int32)


def stacked_normal(key, shape, scale):
    def one_expert(expert_key):
        return (jax.random.normal(expert_key, shape, jnp.float32) * scale).astype(jnp.bfloat16)
    return lax.map(one_expert, jax.random.split(key, EXPERTS))


def setup_inputs(seed: int = 0, part: int = 0) -> dict:
    shared = jax.random.split(jax.random.key(seed), 7)
    own = jax.random.split(jax.random.fold_in(jax.random.key(seed + 1), part), 2)
    x_in = jax.random.normal(own[0], (TOKENS, D_MODEL), jnp.float32).astype(jnp.bfloat16)
    expert_ids = draw_routes(own[1])
    norm_weight = (1.0 + 0.3 * jax.random.normal(shared[0], (D_MODEL,), jnp.float32)).astype(jnp.bfloat16)
    router_w = (jax.random.normal(shared[1], (D_MODEL, EXPERTS), jnp.float32) * D_MODEL ** -0.5).astype(jnp.bfloat16)
    router_b = (0.7 * jax.random.normal(shared[2], (EXPERTS,), jnp.float32)).astype(jnp.bfloat16)
    w_gate_up = stacked_normal(shared[3], (D_MODEL, 2 * D_FF), 5.0 * D_MODEL ** -0.5)
    b_gate_up = jax.random.normal(shared[4], (EXPERTS, 2 * D_FF), jnp.float32).astype(jnp.bfloat16)
    w_down = stacked_normal(shared[5], (D_FF, D_MODEL), 0.125 * D_FF ** -0.5)
    b_down = (0.5 * jax.random.normal(shared[6], (EXPERTS, D_MODEL), jnp.float32)).astype(jnp.bfloat16)
    return dict(x_in=x_in, expert_ids=expert_ids, norm_weight=norm_weight, router_w=router_w, router_b=router_b, w_gate_up=w_gate_up, b_gate_up=b_gate_up, w_down=w_down, b_down=b_down)


def clamped_glu(gate_up):
    gate = jnp.minimum(gate_up[..., 0::2].astype(jnp.float32), LIMIT)
    linear = jnp.clip(gate_up[..., 1::2].astype(jnp.float32), -LIMIT, LIMIT)
    return (gate * jax.nn.sigmoid(ALPHA * gate) * (linear + 1.0)).astype(jnp.bfloat16)


def reference(x_in, expert_ids, norm_weight, router_w, router_b, w_gate_up, b_gate_up, w_down, b_down):
    x_float = x_in.astype(jnp.float32)
    inv_rms = lax.rsqrt(jnp.mean(x_float * x_float, axis=-1, keepdims=True) + EPSILON)
    hidden = (x_float * inv_rms * norm_weight.astype(jnp.float32)).astype(jnp.bfloat16)
    logits = jnp.dot(hidden, router_w, preferred_element_type=jnp.float32) + router_b.astype(jnp.float32)
    gates = jax.nn.softmax(jnp.take_along_axis(logits, expert_ids, axis=1), axis=-1)
    flat_ids = expert_ids.reshape(-1)
    flat_gates = gates.reshape(-1)
    max_rows = GROUP_SIZE * CAPACITY

    def one_expert(combined, weights):
        expert, gate_up_w, gate_up_b, down_w, down_b = weights
        chosen = flat_ids == expert
        picks = jnp.nonzero(chosen, size=max_rows, fill_value=0)[0]
        valid = jnp.arange(max_rows) < jnp.sum(chosen)
        row_token = picks // TOP_K
        rows = hidden[row_token]
        gate_up = (jnp.dot(rows, gate_up_w, preferred_element_type=jnp.float32) + gate_up_b.astype(jnp.float32)).astype(jnp.bfloat16)
        glu_out = clamped_glu(gate_up)
        expert_out = (jnp.dot(glu_out, down_w, preferred_element_type=jnp.float32) + down_b.astype(jnp.float32)).astype(jnp.bfloat16)
        scale = jnp.where(valid, flat_gates[picks], 0.0)
        combined = combined.at[row_token].add(scale[:, None] * expert_out.astype(jnp.float32))
        return combined, None

    start_sum = jnp.zeros((TOKENS, D_MODEL), jnp.float32)
    combined, _ = lax.scan(one_expert, start_sum, (jnp.arange(EXPERTS, dtype=jnp.int32), w_gate_up, b_gate_up, w_down, b_down))
    return (x_float + combined).astype(jnp.bfloat16)
```

```python
import functools

import jax
import jax.numpy as jnp
from jax import lax
from jax.experimental import pallas as pl
from jax.experimental.pallas import tpu as pltpu
from jax.sharding import Mesh, PartitionSpec as P

CAPACITY_FACTOR = 4
EPSILON = 1e-5
LIMIT = 7.0
ALPHA = 1.702
BLOCK = 256
HALF = BLOCK // 2
STEP = 4
RING = ('z', 'y')
ALL = ('z', 'y', 'x', 'c')


def rms_norm(x_in, norm_weight):
    x_float = x_in.astype(jnp.float32)
    inv_rms = lax.rsqrt(jnp.mean(x_float * x_float, axis=-1, keepdims=True) + EPSILON)
    return (x_float * inv_rms * norm_weight.astype(jnp.float32)).astype(jnp.bfloat16)


def route_gates(hidden, expert_ids, router_w, router_b):
    logits = jnp.dot(hidden, router_w, preferred_element_type=jnp.float32) + router_b.astype(jnp.float32)
    chosen = expert_ids[:, :, None] == jnp.arange(logits.shape[1], dtype=jnp.int32)
    return jax.nn.softmax(jnp.sum(jnp.where(chosen, logits[:, None, :], 0.0), axis=-1), axis=-1)


def even_odd(dtype):
    row = lax.broadcasted_iota(jnp.int32, (BLOCK, BLOCK), 0)
    col = lax.broadcasted_iota(jnp.int32, (BLOCK, BLOCK), 1)
    return (row == jnp.where(col < HALF, 2 * col, 2 * (col - HALF) + 1)).astype(jnp.float32).astype(dtype)


def split_kernel(w_ref, low_ref, high_ref):
    perm = even_odd(jnp.bfloat16)
    per_half = low_ref.shape[1] // BLOCK
    for i in range(2 * per_half):
        out = low_ref if i < per_half else high_ref
        part = jnp.dot(w_ref[0, :, i * BLOCK:(i + 1) * BLOCK], perm, preferred_element_type=jnp.float32)
        j = i % per_half
        out[:, j * BLOCK:(j + 1) * BLOCK] = part.astype(jnp.bfloat16)


def split_columns(w):
    _, rows, cols = w.shape
    tile = rows // 4
    return pl.pallas_call(
        split_kernel,
        grid=(4,),
        in_specs=[pl.BlockSpec((1, tile, cols), lambda i: (0, i, 0))],
        out_specs=[pl.BlockSpec((tile, cols // 2), lambda i: (i, 0))] * 2,
        out_shape=[jax.ShapeDtypeStruct((rows, cols // 2), w.dtype)] * 2,
        cost_estimate=pl.CostEstimate(flops=2 * rows * cols * BLOCK, bytes_accessed=4 * rows * cols, transcendentals=0),
        name='split_columns',
    )(w)


def expert_kernel(slot_ref, tok_ref, wd0_ref, wd1_ref, gu0_ref, gu1_ref, bias_ref, out_ref, x_ref, z_ref):
    sources, capacity, d_model = out_ref.shape
    tok_dev = tok_ref.shape[1]
    half_ff = wd0_ref.shape[0]
    lanes = lax.broadcasted_iota(jnp.int32, (capacity, tok_dev), 0)
    for s in range(sources):
        pick = (lanes == slot_ref[s]).astype(jnp.float32).astype(jnp.bfloat16)
        x_ref[s * capacity:(s + 1) * capacity, :] = jnp.dot(pick, tok_ref[s], preferred_element_type=jnp.float32).astype(jnp.bfloat16)
    for i in range(2 * half_ff // HALF):
        w_ref = gu0_ref if i < half_ff // HALF else gu1_ref
        j = i % (half_ff // HALF)
        u = jnp.dot(x_ref[...], w_ref[:, j * BLOCK:(j + 1) * BLOCK], preferred_element_type=jnp.float32)
        u = (u + bias_ref[:, i * BLOCK:(i + 1) * BLOCK].astype(jnp.float32)).astype(jnp.bfloat16).astype(jnp.float32)
        gate = jnp.minimum(u[:, :HALF], LIMIT)
        linear = jnp.clip(u[:, HALF:], -LIMIT, LIMIT)
        z_ref[:, i * HALF:(i + 1) * HALF] = (gate * jax.nn.sigmoid(ALPHA * gate) * (linear + 1.0)).astype(jnp.bfloat16)
    for n in range(0, d_model, 512):
        y = jnp.dot(z_ref[:, :half_ff], wd0_ref[:, n:n + 512], preferred_element_type=jnp.float32)
        y = y + jnp.dot(z_ref[:, half_ff:], wd1_ref[:, n:n + 512], preferred_element_type=jnp.float32)
        y = y + bias_ref[:, 4 * half_ff + n:4 * half_ff + n + 512].astype(jnp.float32)
        out_ref[:, :, n:n + 512] = y.astype(jnp.bfloat16).reshape(sources, capacity, 512)


def run_expert(slot, tokens, weights, bias, capacity):
    sources, tok_dev, d_model = tokens.shape
    half_ff = weights[0].shape[0]
    rows = STEP * capacity
    whole = lambda a: pl.BlockSpec(a.shape, lambda i: (0,) * a.ndim)
    return pl.pallas_call(
        expert_kernel,
        grid=(sources // STEP,),
        in_specs=[pl.BlockSpec((STEP, 1, tok_dev), lambda i: (i, 0, 0)), pl.BlockSpec((STEP, tok_dev, d_model), lambda i: (i, 0, 0))] + [whole(w) for w in weights] + [whole(bias)],
        out_specs=pl.BlockSpec((STEP, capacity, d_model), lambda i: (i, 0, 0)),
        out_shape=jax.ShapeDtypeStruct((sources, capacity, d_model), jnp.bfloat16),
        scratch_shapes=[pltpu.VMEM((rows, d_model), jnp.bfloat16), pltpu.VMEM((rows, 2 * half_ff), jnp.bfloat16)],
        cost_estimate=pl.CostEstimate(flops=2 * sources * capacity * d_model * (6 * half_ff + tok_dev), bytes_accessed=2 * (tokens.size + 6 * half_ff * d_model + sources * capacity * d_model), transcendentals=0),
        name='expert',
    )(slot, tokens, *weights, bias)


def combine_kernel(slot_ref, gate_ref, *refs):
    *y_refs, out_ref, y_all = refs
    experts = len(y_refs)
    capacity = y_refs[0].shape[1]
    tok_dev = slot_ref.shape[2]
    lanes = lax.broadcasted_iota(jnp.int32, (capacity, tok_dev), 0)
    spread = []
    for e in range(experts):
        y_all[e * capacity:(e + 1) * capacity, :] = y_refs[e][0]
        spread.append(jnp.where(lanes == slot_ref[0, e:e + 1, :], gate_ref[0, e:e + 1, :], 0.0))
    spread = jnp.concatenate(spread, axis=0)
    high = spread.astype(jnp.bfloat16)
    rest = spread - high.astype(jnp.float32)
    mid = rest.astype(jnp.bfloat16)
    low = (rest - mid.astype(jnp.float32)).astype(jnp.bfloat16)
    over_slots = (((0,), (0,)), ((), ()))
    for n in range(0, y_all.shape[1], 512):
        y = y_all[:, n:n + 512]
        total = lax.dot_general(low, y, over_slots, preferred_element_type=jnp.float32)
        total = total + lax.dot_general(mid, y, over_slots, preferred_element_type=jnp.float32)
        out_ref[:, n:n + 512] = total + lax.dot_general(high, y, over_slots, preferred_element_type=jnp.float32)


def run_combine(slot, gate, ys):
    sources, experts, tok_dev = slot.shape
    _, capacity, d_model = ys[0].shape
    return pl.pallas_call(
        combine_kernel,
        grid=(sources,),
        in_specs=[pl.BlockSpec((1, experts, tok_dev), lambda i: (i, 0, 0))] * 2 + [pl.BlockSpec((1, capacity, d_model), lambda i: (i, 0, 0))] * experts,
        out_specs=pl.BlockSpec((tok_dev, d_model), lambda i: (i, 0)),
        out_shape=jax.ShapeDtypeStruct((sources * tok_dev, d_model), jnp.float32),
        scratch_shapes=[pltpu.VMEM((experts * capacity, d_model), jnp.bfloat16)],
        cost_estimate=pl.CostEstimate(flops=6 * sources * tok_dev * experts * capacity * d_model, bytes_accessed=sources * d_model * (2 * experts * capacity + 4 * tok_dev), transcendentals=0),
        name='combine',
    )(slot, gate, *ys)


def solution(mesh):
    torus = Mesh(mesh.devices.reshape(4, 4, 4, 2), ALL)
    rows_spec = P(ALL, None)
    plus = [(i, (i + 1) % 4) for i in range(4)]
    minus = [(i, (i + 3) % 4) for i in range(4)]
    swap = [(0, 1), (1, 0)]

    def local_block(x_in, expert_ids, norm_weight, router_w, router_b, w_gate_up, b_gate_up, w_down, b_down):
        tok_dev, d_model = x_in.shape
        top_k = expert_ids.shape[1]
        capacity = CAPACITY_FACTOR * top_k * tok_dev // 128
        d_ff = w_down.shape[1]
        zi, yi, xi, ci = (lax.axis_index(a) for a in ALL)
        first = (zi * 4 + yi) * 8

        b_split = jnp.einsum('rbk,kc->rbc', b_gate_up.reshape(1, -1, BLOCK), even_odd(jnp.bfloat16), preferred_element_type=jnp.bfloat16).reshape(1, -1)
        own = [w_down[0, :d_ff // 2], w_down[0, d_ff // 2:], *split_columns(w_gate_up), jnp.concatenate([b_split, b_down], axis=1)]
        left = [lax.ppermute(w, 'x', plus) for w in own]
        right = [lax.ppermute(w, 'x', minus) for w in own]
        far = [lax.ppermute(left[i], 'x', plus) if i % 2 == 0 else lax.ppermute(right[i], 'x', minus) for i in range(5)]
        sets = [(0, own), (3, left), (1, right), (2, far)]

        hidden = rms_norm(x_in, norm_weight)
        tokens = lax.all_gather(hidden, RING, axis=0, tiled=False).reshape(16, tok_dev, d_model)
        gates = route_gates(hidden, expert_ids, router_w, router_b)
        info = lax.all_gather(jnp.concatenate([expert_ids.T.astype(jnp.float32), gates.T], axis=0), RING, axis=0, tiled=False).reshape(16, 2 * top_k, tok_dev)
        ids, gates = info[:, :top_k].astype(jnp.int32), info[:, top_k:]

        experts = first + jnp.stack([((xi + step) % 4) * 2 + (ci if same else 1 - ci) for step, _ in sets for same in (True, False)])
        match = ids[:, None, :, :] == experts[None, :, None, None]
        member = jnp.any(match, axis=2)
        gate = jnp.sum(jnp.where(match, gates[:, None, :, :], 0.0), axis=2)
        before = (jnp.arange(tok_dev)[:, None] < jnp.arange(tok_dev)[None, :]).astype(jnp.bfloat16)
        rank = jnp.einsum('seu,ut->set', member.astype(jnp.bfloat16), before, preferred_element_type=jnp.float32).astype(jnp.int32)
        slot = jnp.where(member, rank, -1)

        ys = []
        for pair, (_, weights) in enumerate(sets):
            other = [lax.ppermute(w, 'c', swap) for w in weights]
            for which, (*mats, bias) in enumerate((weights, other)):
                e = 2 * pair + which
                ys.append(run_expert(slot[:, e:e + 1, :], tokens, mats, bias, capacity))
        partial = run_combine(slot, gate, ys)
        mixed = lax.psum_scatter(partial, RING, scatter_dimension=0, tiled=True)
        return (x_in.astype(jnp.float32) + mixed).astype(jnp.bfloat16)

    w3, w2 = P(ALL, None, None), P(ALL, None)
    return jax.shard_map(local_block, mesh=torus, in_specs=(rows_spec, rows_spec, P(), P(), P(), w3, w2, w3, w2), out_specs=rows_spec, check_vma=False)
```

```python
import functools

import jax
import jax.numpy as jnp
from jax import lax
from jax.experimental import pallas as pl
from jax.experimental.pallas import tpu as pltpu
from jax.sharding import Mesh, PartitionSpec as P


CAPACITY_FACTOR = 4
EPSILON = 1e-5
LIMIT = 7.0
ALPHA = 1.702
BLOCK = 256
HALF = BLOCK // 2
STEPS = 2
PARTS = 2
RING = ('z', 'y')
ALL = ('z', 'y', 'x', 'c')


def rms_norm(x_in, norm_weight):
    x_float = x_in.astype(jnp.float32)
    inv_rms = lax.rsqrt(jnp.mean(x_float * x_float, axis=-1, keepdims=True) + EPSILON)
    return (x_float * inv_rms * norm_weight.astype(jnp.float32)).astype(jnp.bfloat16)


def route_gates(hidden, expert_ids, router_w, router_b):
    logits = jnp.dot(hidden, router_w, preferred_element_type=jnp.float32) + router_b.astype(jnp.float32)
    chosen = expert_ids[:, :, None] == jnp.arange(logits.shape[1], dtype=jnp.int32)
    return jax.nn.softmax(jnp.sum(jnp.where(chosen, logits[:, None, :], 0.0), axis=-1), axis=-1)


def even_odd(dtype):
    row = lax.broadcasted_iota(jnp.int32, (BLOCK, BLOCK), 0)
    col = lax.broadcasted_iota(jnp.int32, (BLOCK, BLOCK), 1)
    return (row == jnp.where(col < HALF, 2 * col, 2 * (col - HALF) + 1)).astype(jnp.float32).astype(dtype)


def split_kernel(w_ref, low_ref, high_ref):
    perm = even_odd(jnp.bfloat16)
    per_half = low_ref.shape[1] // BLOCK
    for i in range(2 * per_half):
        out = low_ref if i < per_half else high_ref
        part = jnp.dot(w_ref[0, :, i * BLOCK:(i + 1) * BLOCK], perm, preferred_element_type=jnp.float32)
        j = i % per_half
        out[:, j * BLOCK:(j + 1) * BLOCK] = part.astype(jnp.bfloat16)


def split_columns(w):
    _, rows, cols = w.shape
    tile = rows // 4
    return pl.pallas_call(
        split_kernel,
        grid=(4,),
        in_specs=[pl.BlockSpec((1, tile, cols), lambda i: (0, i, 0))],
        out_specs=[pl.BlockSpec((tile, cols // 2), lambda i: (i, 0))] * 2,
        out_shape=[jax.ShapeDtypeStruct((rows, cols // 2), w.dtype)] * 2,
        cost_estimate=pl.CostEstimate(flops=2 * rows * cols * BLOCK, bytes_accessed=4 * rows * cols, transcendentals=0),
        name='split_columns',
    )(w)


def pick_kernel(slot_ref, tok_ref, out_ref):
    experts, _, capacity, _ = out_ref.shape
    lanes = lax.broadcasted_iota(jnp.int32, (capacity, tok_ref.shape[1]), 0)
    picks = jnp.concatenate([(lanes == slot_ref[0, e:e + 1, :]).astype(jnp.float32) for e in range(experts)], axis=0).astype(jnp.bfloat16)
    for n in range(0, tok_ref.shape[2], 512):
        rows = jnp.dot(picks, tok_ref[0, :, n:n + 512], preferred_element_type=jnp.float32).astype(jnp.bfloat16)
        for e in range(experts):
            out_ref[e, 0, :, n:n + 512] = rows[e * capacity:(e + 1) * capacity]


def pick_rows(slot, tokens, capacity):
    sources, experts, tok_dev = slot.shape
    d_model = tokens.shape[2]
    return pl.pallas_call(
        pick_kernel,
        grid=(sources,),
        in_specs=[pl.BlockSpec((1, experts, tok_dev), lambda i: (i, 0, 0)), pl.BlockSpec((1, tok_dev, d_model), lambda i: (i, 0, 0))],
        out_specs=pl.BlockSpec((experts, 1, capacity, d_model), lambda i: (0, i, 0, 0)),
        out_shape=jax.ShapeDtypeStruct((experts, sources, capacity, d_model), jnp.bfloat16),
        cost_estimate=pl.CostEstimate(flops=2 * sources * experts * capacity * tok_dev * d_model, bytes_accessed=2 * sources * d_model * (tok_dev + experts * capacity), transcendentals=0),
        name='pick_rows',
    )(slot, tokens)


def expert_kernel(x_ref, wd0_ref, wd1_ref, gu0_ref, gu1_ref, bias_ref, out_ref, z_ref):
    _, d_model = out_ref.shape
    half_ff = wd0_ref.shape[0]
    perm = even_odd(jnp.bfloat16)
    for i in range(2 * half_ff // HALF):
        w_ref = gu0_ref if i < half_ff // HALF else gu1_ref
        j = i % (half_ff // HALF)
        u = jnp.dot(x_ref[0], w_ref[:, j * BLOCK:(j + 1) * BLOCK], preferred_element_type=jnp.float32)
        b = jnp.broadcast_to(bias_ref[:, i * BLOCK:(i + 1) * BLOCK].astype(jnp.float32), (16, BLOCK)).astype(jnp.bfloat16)
        b = jnp.dot(b, perm, preferred_element_type=jnp.float32)[0:1]
        u = (u + b).astype(jnp.bfloat16).astype(jnp.float32)
        gate = jnp.minimum(u[:, :HALF], LIMIT)
        linear = jnp.clip(u[:, HALF:], -LIMIT, LIMIT)
        z_ref[:, i * HALF:(i + 1) * HALF] = (gate * jax.nn.sigmoid(ALPHA * gate) * (linear + 1.0)).astype(jnp.bfloat16)
    for n in range(0, d_model, 256):
        y = jnp.dot(z_ref[:, :half_ff], wd0_ref[:, n:n + 256], preferred_element_type=jnp.float32)
        y = y + jnp.dot(z_ref[:, half_ff:], wd1_ref[:, n:n + 256], preferred_element_type=jnp.float32)
        y = y + bias_ref[:, 4 * half_ff + n:4 * half_ff + n + 256].astype(jnp.float32)
        out_ref[:, n:n + 256] = y.astype(jnp.bfloat16)


def run_expert(e, rows, weights, bias):
    total, d_model = rows.shape[1:]
    half_ff = weights[0].shape[0]
    tile = total // STEPS
    whole = lambda a: pl.BlockSpec(a.shape, lambda i: (0,) * a.ndim)
    return pl.pallas_call(
        expert_kernel,
        grid=(STEPS,),
        in_specs=[pl.BlockSpec((1, tile, d_model), lambda i: (e, i, 0))] + [whole(w) for w in weights] + [whole(bias)],
        out_specs=pl.BlockSpec((tile, d_model), lambda i: (i, 0)),
        out_shape=jax.ShapeDtypeStruct((total, d_model), jnp.bfloat16),
        scratch_shapes=[pltpu.VMEM((tile, 2 * half_ff), jnp.bfloat16)],
        cost_estimate=pl.CostEstimate(flops=12 * total * d_model * half_ff, bytes_accessed=4 * (3 * half_ff * d_model + total * d_model), transcendentals=0),
        name='expert',
    )(rows, *weights, bias)


def combine_kernel(slot_ref, gate_ref, *refs, experts, add):
    y_refs = refs[:len(experts)]
    old_ref = refs[len(experts)] if add else None
    out_ref, y_all = refs[-2:]
    capacity = y_refs[0].shape[1]
    tok_dev = slot_ref.shape[2]
    lanes = lax.broadcasted_iota(jnp.int32, (capacity, tok_dev), 0)
    spread = []
    for i, e in enumerate(experts):
        y_all[i * capacity:(i + 1) * capacity, :] = y_refs[i][0]
        spread.append(jnp.where(lanes == slot_ref[0, e:e + 1, :], gate_ref[0, e:e + 1, :], 0.0))
    spread = jnp.concatenate(spread, axis=0)
    high = spread.astype(jnp.bfloat16)
    rest = spread - high.astype(jnp.float32)
    mid = rest.astype(jnp.bfloat16)
    low = (rest - mid.astype(jnp.float32)).astype(jnp.bfloat16)
    over_slots = (((0,), (0,)), ((), ()))
    for n in range(0, y_all.shape[1], 512):
        y = y_all[:, n:n + 512]
        total = lax.dot_general(low, y, over_slots, preferred_element_type=jnp.float32)
        total = total + lax.dot_general(mid, y, over_slots, preferred_element_type=jnp.float32)
        total = total + lax.dot_general(high, y, over_slots, preferred_element_type=jnp.float32)
        out_ref[:, n:n + 512] = old_ref[:, n:n + 512] + total if add else total


def run_combine(slot, gate, ys, experts, part, old=None):
    sources, count, tok_dev = slot.shape
    capacity = ys[0].shape[0] // sources
    ys = [y.reshape(sources, capacity, -1) for y in ys]
    cols = ys[0].shape[2] // PARTS
    extra = [] if old is None else [old]
    return pl.pallas_call(
        functools.partial(combine_kernel, experts=experts, add=bool(extra)),
        grid=(sources,),
        in_specs=[pl.BlockSpec((1, count, tok_dev), lambda i: (i, 0, 0))] * 2
        + [pl.BlockSpec((1, capacity, cols), lambda i: (i, 0, part))] * len(ys)
        + [pl.BlockSpec((tok_dev, cols), lambda i: (i, 0))] * len(extra),
        out_specs=pl.BlockSpec((tok_dev, cols), lambda i: (i, 0)),
        out_shape=jax.ShapeDtypeStruct((sources * tok_dev, cols), jnp.float32),
        scratch_shapes=[pltpu.VMEM((len(ys) * capacity, cols), jnp.bfloat16)],
        cost_estimate=pl.CostEstimate(flops=6 * sources * tok_dev * len(ys) * capacity * cols, bytes_accessed=sources * cols * (2 * len(ys) * capacity + 4 * tok_dev * (1 + len(extra))), transcendentals=0),
        name='combine',
    )(slot, gate, *ys, *extra)


def solution(mesh):
    torus = Mesh(mesh.devices.reshape(4, 4, 4, 2), ALL)
    rows_spec = P(ALL, None)
    plus = [(i, (i + 1) % 4) for i in range(4)]
    minus = [(i, (i + 3) % 4) for i in range(4)]
    swap = [(0, 1), (1, 0)]

    def local_block(x_in, expert_ids, norm_weight, router_w, router_b, w_gate_up, b_gate_up, w_down, b_down):
        tok_dev, d_model = x_in.shape
        top_k = expert_ids.shape[1]
        capacity = CAPACITY_FACTOR * top_k * tok_dev // 128
        d_ff = w_down.shape[1]
        zi, yi, xi, ci = (lax.axis_index(a) for a in ALL)
        first = (zi * 4 + yi) * 8

        own = [w_down[0, :d_ff // 2], w_down[0, d_ff // 2:], *split_columns(w_gate_up), jnp.concatenate([b_gate_up, b_down], axis=1)]
        left = [lax.ppermute(w, 'x', plus) for w in own]
        right = [lax.ppermute(w, 'x', minus) for w in own]
        far = [lax.ppermute(left[i], 'x', plus) if i % 2 == 0 else lax.ppermute(right[i], 'x', minus) for i in range(5)]
        sets = [(0, own), (3, left), (1, right), (2, far)]

        hidden = rms_norm(x_in, norm_weight)
        tokens = lax.all_gather(hidden, RING, axis=0, tiled=False).reshape(16, tok_dev, d_model)
        gates = route_gates(hidden, expert_ids, router_w, router_b)
        info = lax.all_gather(jnp.concatenate([expert_ids.T.astype(jnp.float32), gates.T], axis=0), RING, axis=0, tiled=False).reshape(16, 2 * top_k, tok_dev)
        ids, gates = info[:, :top_k].astype(jnp.int32), info[:, top_k:]

        experts = first + jnp.stack([((xi + step) % 4) * 2 + (ci if same else 1 - ci) for step, _ in sets for same in (True, False)])
        match = ids[:, None, :, :] == experts[None, :, None, None]
        member = jnp.any(match, axis=2)
        gate = jnp.sum(jnp.where(match, gates[:, None, :, :], 0.0), axis=2)
        before = (jnp.arange(tok_dev)[:, None] < jnp.arange(tok_dev)[None, :]).astype(jnp.bfloat16)
        rank = jnp.einsum('seu,ut->set', member.astype(jnp.bfloat16), before, preferred_element_type=jnp.float32).astype(jnp.int32)
        slot = jnp.where(member, rank, -1)

        rows = pick_rows(slot, tokens, capacity).reshape(8, 16 * capacity, d_model)
        ys = []
        for _, weights in sets:
            other = [lax.ppermute(w, 'c', swap) for w in weights]
            for *mats, bias in (weights, other):
                ys.append(run_expert(len(ys), rows, mats, bias))
        mixed = []
        for part in range(PARTS):
            early = run_combine(slot, gate, ys[:6], range(6), part)
            late = run_combine(slot, gate, ys[6:], range(6, 8), part, early)
            mixed.append(lax.psum_scatter(late, RING, scatter_dimension=0, tiled=True))
        return (x_in.astype(jnp.float32) + jnp.concatenate(mixed, axis=1)).astype(jnp.bfloat16)

    w3, w2 = P(ALL, None, None), P(ALL, None)
    return jax.shard_map(local_block, mesh=torus, in_specs=(rows_spec, rows_spec, P(), P(), P(), w3, w2, w3, w2), out_specs=rows_spec, check_vma=False)
```

```python
import functools

import jax
import jax.numpy as jnp
from jax import lax
from jax.experimental import pallas as pl
from jax.experimental.pallas import tpu as pltpu
from jax.sharding import Mesh, PartitionSpec as P


CAPACITY_FACTOR = 4
EPSILON = 1e-5
LIMIT = 7.0
ALPHA = 1.702
BLOCK = 256
HALF = BLOCK // 2
GROUP = 2
GATE_JOBS = {
    'za': ((0, 0), (0, 1), (1, 0), (1, 1)),
    'zb': ((2, 0), (4, 1), (3, 0), (5, 1)),
    'zc': ((2, 1), (4, 0), (3, 1), (5, 0)),
    'zd': ((6, 0), (6, 1), (7, 0), (7, 1)),
}
DOWN_JOBS = {'ya': (0, 1), 'yb': (2, 4), 'yc': (3, 5)}
RING = ('z', 'y')
ALL = ('z', 'y', 'x', 'c')


def rms_norm(x_in, norm_weight):
    x_float = x_in.astype(jnp.float32)
    inv_rms = lax.rsqrt(jnp.mean(x_float * x_float, axis=-1, keepdims=True) + EPSILON)
    return (x_float * inv_rms * norm_weight.astype(jnp.float32)).astype(jnp.bfloat16)


def route_gates(hidden, expert_ids, router_w, router_b):
    logits = jnp.dot(hidden, router_w, preferred_element_type=jnp.float32) + router_b.astype(jnp.float32)
    chosen = expert_ids[:, :, None] == jnp.arange(logits.shape[1], dtype=jnp.int32)
    return jax.nn.softmax(jnp.sum(jnp.where(chosen, logits[:, None, :], 0.0), axis=-1), axis=-1)


def even_odd(dtype):
    row = lax.broadcasted_iota(jnp.int32, (BLOCK, BLOCK), 0)
    col = lax.broadcasted_iota(jnp.int32, (BLOCK, BLOCK), 1)
    return (row == jnp.where(col < HALF, 2 * col, 2 * (col - HALF) + 1)).astype(jnp.float32).astype(dtype)


def split_kernel(w_ref, low_ref, high_ref):
    perm = even_odd(jnp.bfloat16)
    per_half = low_ref.shape[1] // BLOCK
    for i in range(2 * per_half):
        out = low_ref if i < per_half else high_ref
        part = jnp.dot(w_ref[0, :, i * BLOCK:(i + 1) * BLOCK], perm, preferred_element_type=jnp.float32)
        j = i % per_half
        out[:, j * BLOCK:(j + 1) * BLOCK] = part.astype(jnp.bfloat16)


def split_columns(w):
    _, rows, cols = w.shape
    tile = rows // 4
    return pl.pallas_call(
        split_kernel,
        grid=(4,),
        in_specs=[pl.BlockSpec((1, tile, cols), lambda i: (0, i, 0))],
        out_specs=[pl.BlockSpec((tile, cols // 2), lambda i: (i, 0))] * 2,
        out_shape=[jax.ShapeDtypeStruct((rows, cols // 2), w.dtype)] * 2,
        cost_estimate=pl.CostEstimate(flops=2 * rows * cols * BLOCK, bytes_accessed=4 * rows * cols, transcendentals=0),
        name='split_columns',
    )(w)


def pick_kernel(slot_ref, tok_ref, out_ref):
    experts, _, capacity, _ = out_ref.shape
    lanes = lax.broadcasted_iota(jnp.int32, (capacity, tok_ref.shape[1]), 0)
    picks = jnp.concatenate([(lanes == slot_ref[0, e:e + 1, :]).astype(jnp.float32) for e in range(experts)], axis=0).astype(jnp.bfloat16)
    for n in range(0, tok_ref.shape[2], 512):
        rows = jnp.dot(picks, tok_ref[0, :, n:n + 512], preferred_element_type=jnp.float32).astype(jnp.bfloat16)
        for e in range(experts):
            out_ref[e, 0, :, n:n + 512] = rows[e * capacity:(e + 1) * capacity]


def pick_rows(slot, tokens, capacity):
    sources, experts, tok_dev = slot.shape
    d_model = tokens.shape[2]
    return pl.pallas_call(
        pick_kernel,
        grid=(sources,),
        in_specs=[pl.BlockSpec((1, experts, tok_dev), lambda i: (i, 0, 0)), pl.BlockSpec((1, tok_dev, d_model), lambda i: (i, 0, 0))],
        out_specs=pl.BlockSpec((experts, 1, capacity, d_model), lambda i: (0, i, 0, 0)),
        out_shape=jax.ShapeDtypeStruct((experts, sources, capacity, d_model), jnp.bfloat16),
        cost_estimate=pl.CostEstimate(flops=2 * sources * experts * capacity * tok_dev * d_model, bytes_accessed=2 * sources * d_model * (tok_dev + experts * capacity), transcendentals=0),
        name='pick_rows',
    )(slot, tokens)


def gate_up_kernel(x_ref, *refs, jobs):
    w_refs, bias_refs, out_refs = refs[:jobs], refs[jobs:2 * jobs], refs[2 * jobs:]
    steps = pl.num_programs(0) // jobs
    for j in range(jobs):
        @pl.when(pl.program_id(0) // steps == j)
        def _():
            perm = even_odd(jnp.bfloat16)
            bias = jnp.broadcast_to(bias_refs[j][...].astype(jnp.float32), (16, BLOCK)).astype(jnp.bfloat16)
            bias = jnp.dot(bias, perm, preferred_element_type=jnp.float32)[0:1]
            u = jnp.dot(x_ref[0], w_refs[j][...], preferred_element_type=jnp.float32)
            u = (u + bias).astype(jnp.bfloat16).astype(jnp.float32)
            gate = jnp.minimum(u[:, :HALF], LIMIT)
            linear = jnp.clip(u[:, HALF:], -LIMIT, LIMIT)
            out_refs[j][...] = (gate * jax.nn.sigmoid(ALPHA * gate) * (linear + 1.0)).astype(jnp.bfloat16)


def gate_up(rows, jobs):
    total, d_model = rows.shape[1:]
    steps = jobs[0][2].shape[1] // BLOCK

    def block(j, i):
        return jnp.clip(i - j * steps, 0, steps - 1)

    def expert(i):
        return sum(jnp.where(i // steps == j, job[0], 0) for j, job in enumerate(jobs))

    count = len(jobs)
    return pl.pallas_call(
        functools.partial(gate_up_kernel, jobs=count),
        grid=(count * steps,),
        in_specs=[pl.BlockSpec((1, total, d_model), lambda i: (expert(i), 0, 0))]
        + [pl.BlockSpec((d_model, BLOCK), lambda i, j=j: (0, block(j, i))) for j in range(count)]
        + [pl.BlockSpec((1, BLOCK), lambda i, j=j: (0, jobs[j][1] * steps + block(j, i))) for j in range(count)],
        out_specs=[pl.BlockSpec((total, HALF), lambda i, j=j: (0, block(j, i))) for j in range(count)],
        out_shape=[jax.ShapeDtypeStruct((total, steps * HALF), jnp.bfloat16)] * count,
        cost_estimate=pl.CostEstimate(flops=2 * count * total * jobs[0][2].size, bytes_accessed=2 * count * (jobs[0][2].size + total * d_model), transcendentals=0),
        name='gate_up',
    )(rows, *[job[2] for job in jobs], *[job[3] for job in jobs])


def down_kernel(*refs, jobs):
    ins, out_refs = refs[:4 * jobs], refs[4 * jobs:]
    steps = pl.num_programs(0) // jobs
    for j in range(jobs):
        z0_ref, z1_ref, w_ref, bias_ref = ins[4 * j:4 * j + 4]

        @pl.when(pl.program_id(0) // steps == j)
        def _():
            z = jnp.concatenate([z0_ref[...], z1_ref[...]], axis=1)
            y = jnp.dot(z, w_ref[...], preferred_element_type=jnp.float32)
            out_refs[j][...] = (y + bias_ref[...].astype(jnp.float32)).astype(jnp.bfloat16)


def down(jobs):
    total, half_ff = jobs[0][0].shape
    d_ff, d_model = jobs[0][2].shape
    tile = 512
    steps, first, count = d_model // tile, 2 * d_ff // tile, len(jobs)

    def block(j, i):
        return jnp.clip(i - j * steps, 0, steps - 1)

    in_specs = []
    for j in range(count):
        in_specs += [pl.BlockSpec((total, half_ff), lambda i: (0, 0))] * 2
        in_specs += [pl.BlockSpec((d_ff, tile), lambda i, j=j: (0, block(j, i))), pl.BlockSpec((1, tile), lambda i, j=j: (0, first + block(j, i)))]
    return pl.pallas_call(
        functools.partial(down_kernel, jobs=count),
        grid=(count * steps,),
        in_specs=in_specs,
        out_specs=[pl.BlockSpec((total, tile), lambda i, j=j: (0, block(j, i))) for j in range(count)],
        out_shape=[jax.ShapeDtypeStruct((total, d_model), jnp.bfloat16)] * count,
        cost_estimate=pl.CostEstimate(flops=2 * count * total * d_ff * d_model, bytes_accessed=2 * count * (d_ff * d_model + total * d_model), transcendentals=0),
        name='down',
    )(*[a for job in jobs for a in job])


def gate_terms(slot, gate, experts, capacity):
    lanes = lax.broadcasted_iota(jnp.int32, (capacity, slot.shape[1]), 0)
    spread = jnp.concatenate([jnp.where(lanes == slot[e:e + 1, :], gate[e:e + 1, :], 0.0) for e in experts], axis=0).T
    high = spread.astype(jnp.bfloat16)
    rest = spread - high.astype(jnp.float32)
    mid = rest.astype(jnp.bfloat16)
    low = (rest - mid.astype(jnp.float32)).astype(jnp.bfloat16)
    return jnp.concatenate([low, mid, high], axis=1)


def early_kernel(slot_ref, gate_ref, *refs, experts):
    *y_refs, out_ref, y_all = refs
    capacity = y_refs[0].shape[1]
    count = len(experts) * capacity
    for i in range(len(experts)):
        for term in range(3):
            y_all[term * count + i * capacity:term * count + (i + 1) * capacity, :] = y_refs[i][0]
    terms = gate_terms(slot_ref[0], gate_ref[0], experts, capacity)
    for n in range(0, y_all.shape[1], 512):
        out_ref[:, n:n + 512] = jnp.dot(terms, y_all[:, n:n + 512], preferred_element_type=jnp.float32)


def early_sum(slot, gate, ys, experts):
    sources, count, tok_dev = slot.shape
    capacity, d_model = ys[0].shape[0] // sources, ys[0].shape[1]
    return pl.pallas_call(
        functools.partial(early_kernel, experts=experts),
        grid=(sources,),
        in_specs=[pl.BlockSpec((1, count, tok_dev), lambda i: (i, 0, 0))] * 2 + [pl.BlockSpec((1, capacity, d_model), lambda i: (i, 0, 0))] * len(ys),
        out_specs=pl.BlockSpec((tok_dev, d_model), lambda i: (i, 0)),
        out_shape=jax.ShapeDtypeStruct((sources * tok_dev, d_model), jnp.float32),
        scratch_shapes=[pltpu.VMEM((3 * len(ys) * capacity, d_model), jnp.bfloat16)],
        cost_estimate=pl.CostEstimate(flops=6 * sources * tok_dev * len(ys) * capacity * d_model, bytes_accessed=sources * d_model * (2 * len(ys) * capacity + 4 * tok_dev), transcendentals=0),
        name='early_sum',
    )(slot, gate, *[y.reshape(sources, capacity, d_model) for y in ys])


def late_kernel(slot_ref, gate_ref, za0, za1, zb0, zb1, wa0, wa1, wb0, wb1, bias_a, bias_b, old_ref, out_ref, y_all, w_all, *, experts):
    group, capacity = GROUP, za0.shape[0] // (2 * GROUP)
    tok_dev = slot_ref.shape[2]
    d_model = out_ref.shape[1]
    first = bias_a.shape[1] - d_model
    count = len(experts) * capacity
    part = lax.rem(pl.program_id(0), 2)

    half_ff = wa0.shape[0]

    @pl.when(pl.program_id(0) == 0)
    def _():
        for i, (w0, w1) in enumerate(((wa0, wa1), (wb0, wb1))):
            w_all[i, :half_ff] = w0[...]
            w_all[i, half_ff:] = w1[...]

    @pl.when(part == 0)
    def _():
        for i, (z0, z1, bias) in enumerate(((za0, za1, bias_a), (zb0, zb1, bias_b))):
            z = jnp.concatenate([z0[...], z1[...]], axis=1)
            for n in range(0, d_model, 512):
                y = jnp.dot(z, w_all[i, :, n:n + 512], preferred_element_type=jnp.float32)
                y = (y + bias[:, first + n:first + n + 512].astype(jnp.float32)).astype(jnp.bfloat16)
                for s in range(2 * group):
                    for term in range(3):
                        y_all[s, term * count + i * capacity:term * count + (i + 1) * capacity, n:n + 512] = y[s * capacity:(s + 1) * capacity]

    for s in range(group):
        terms = gate_terms(slot_ref[s], gate_ref[s], experts, capacity)
        for n in range(0, d_model, 512):
            rows = pl.ds(s * tok_dev, tok_dev)
            out_ref[rows, n:n + 512] = old_ref[rows, n:n + 512] + jnp.dot(terms, y_all[part * group + s, :, n:n + 512], preferred_element_type=jnp.float32)


def late_sum(slot, gate, zs, weights, biases, experts, old):
    sources, count, tok_dev = slot.shape
    total, half_ff = zs[0].shape
    d_model = old.shape[1]
    capacity = total // sources
    whole = lambda a: pl.BlockSpec(a.shape, lambda i: (0, 0))
    return pl.pallas_call(
        functools.partial(late_kernel, experts=experts),
        grid=(sources // GROUP,),
        in_specs=[pl.BlockSpec((GROUP, count, tok_dev), lambda i: (i, 0, 0))] * 2
        + [pl.BlockSpec((2 * GROUP * capacity, half_ff), lambda i: (i // 2, 0))] * 4
        + [whole(w) for w in weights] + [whole(b) for b in biases]
        + [pl.BlockSpec((GROUP * tok_dev, d_model), lambda i: (i, 0))],
        out_specs=pl.BlockSpec((GROUP * tok_dev, d_model), lambda i: (i, 0)),
        out_shape=jax.ShapeDtypeStruct(old.shape, jnp.float32),
        scratch_shapes=[pltpu.VMEM((2 * GROUP, 3 * len(experts) * capacity, d_model), jnp.bfloat16), pltpu.VMEM((len(experts), 2 * half_ff, d_model), jnp.bfloat16)],
        cost_estimate=pl.CostEstimate(flops=2 * total * 4 * half_ff * d_model + 6 * old.size * len(experts) * capacity, bytes_accessed=8 * old.size, transcendentals=0),
        name='late_sum',
    )(slot, gate, *zs, *weights, *biases, old)


def solution(mesh):
    torus = Mesh(mesh.devices.reshape(4, 4, 4, 2), ALL)
    rows_spec = P(ALL, None)
    plus = [(i, (i + 1) % 4) for i in range(4)]
    minus = [(i, (i + 3) % 4) for i in range(4)]
    swap = [(0, 1), (1, 0)]

    def local_block(x_in, expert_ids, norm_weight, router_w, router_b, w_gate_up, b_gate_up, w_down, b_down):
        tok_dev, d_model = x_in.shape
        top_k = expert_ids.shape[1]
        capacity = CAPACITY_FACTOR * top_k * tok_dev // 128
        d_ff = w_down.shape[1]
        zi, yi, xi, ci = (lax.axis_index(a) for a in ALL)
        first = (zi * 4 + yi) * 8

        gu0, gu1 = split_columns(w_gate_up)
        own = dict(wd=w_down[0], gu0=gu0, gu1=gu1, b=jnp.concatenate([b_gate_up, b_down], axis=1))
        left = {k: lax.ppermute(w, 'x', plus) for k, w in own.items()}
        right = {k: lax.ppermute(w, 'x', minus) for k, w in own.items()}
        far = dict(
            gu0=lax.ppermute(left['gu0'], 'x', plus),
            gu1=lax.ppermute(right['gu1'], 'x', minus),
            wd0=lax.ppermute(left['wd'][:d_ff // 2], 'x', plus),
            wd1=lax.ppermute(right['wd'][d_ff // 2:], 'x', minus),
            b=lax.ppermute(left['b'], 'x', plus),
        )
        sets = [(0, own), (3, left), (1, right), (2, far)]

        hidden = rms_norm(x_in, norm_weight)
        tokens = lax.all_gather(hidden, RING, axis=0, tiled=False).reshape(16, tok_dev, d_model)
        gates = route_gates(hidden, expert_ids, router_w, router_b)
        info = lax.all_gather(jnp.concatenate([expert_ids.T.astype(jnp.float32), gates.T], axis=0), RING, axis=0, tiled=False).reshape(16, 2 * top_k, tok_dev)
        ids, gates = info[:, :top_k].astype(jnp.int32), info[:, top_k:]

        experts = first + jnp.stack([((xi + step) % 4) * 2 + (ci if same else 1 - ci) for step, _ in sets for same in (True, False)])
        match = ids[:, None, :, :] == experts[None, :, None, None]
        member = jnp.any(match, axis=2)
        gate = jnp.sum(jnp.where(match, gates[:, None, :, :], 0.0), axis=2)
        before = (jnp.arange(tok_dev)[:, None] < jnp.arange(tok_dev)[None, :]).astype(jnp.bfloat16)
        rank = jnp.einsum('seu,ut->set', member.astype(jnp.bfloat16), before, preferred_element_type=jnp.float32).astype(jnp.int32)
        slot = jnp.where(member, rank, -1)

        rows = pick_rows(slot, tokens, capacity).reshape(8, 16 * capacity, d_model)
        held = []
        for _, weights in sets:
            held += [weights, {k: lax.ppermute(w, 'c', swap) for k, w in weights.items()}]
        z = {}
        for jobs in GATE_JOBS.values():
            done = gate_up(rows, [(e, i, held[e]['gu%d' % i], held[e]['b']) for e, i in jobs])
            z.update(zip(jobs, done))
        ys = {}
        for jobs in DOWN_JOBS.values():
            ys.update(zip(jobs, down([(z[e, 0], z[e, 1], held[e]['wd'], held[e]['b']) for e in jobs])))
        ys = [ys[e] for e in range(6)]
        last = [z[e, i] for e in (6, 7) for i in (0, 1)]
        early = early_sum(slot, gate, ys, range(6))
        total = late_sum(slot, gate, last, [held[e]['wd%d' % i] for e in (6, 7) for i in (0, 1)], [held[6]['b'], held[7]['b']], range(6, 8), early)
        mixed = lax.psum_scatter(total, RING, scatter_dimension=0, tiled=True)
        return (x_in.astype(jnp.float32) + mixed).astype(jnp.bfloat16)

    w3, w2 = P(ALL, None, None), P(ALL, None)
    return jax.shard_map(local_block, mesh=torus, in_specs=(rows_spec, rows_spec, P(), P(), P(), w3, w2, w3, w2), out_specs=rows_spec, check_vma=False)
```

```python
import functools

import jax
import jax.numpy as jnp
from jax import lax
from jax.experimental import pallas as pl
from jax.experimental.pallas import tpu as pltpu
from jax.sharding import Mesh, PartitionSpec as P


CAPACITY_FACTOR = 4
EPSILON = 1e-5
LIMIT = 7.0
ALPHA = 1.702
BLOCK = 256
HALF = BLOCK // 2
GROUP = 2
GATE_JOBS = {
    'za': ((0, 0), (0, 1), (1, 0), (1, 1)),
    'zb': ((2, 0), (4, 1), (3, 0), (5, 1)),
    'zc': ((2, 1), (4, 0), (3, 1), (5, 0)),
    'zd': ((6, 0), (6, 1)),
    'ze': ((7, 0), (7, 1)),
}
DOWN_JOBS = {'ya': (0, 1), 'yb': (2, 4), 'yc': (3, 5)}
RING = ('z', 'y')
ALL = ('z', 'y', 'x', 'c')


def rms_norm(x_in, norm_weight):
    x_float = x_in.astype(jnp.float32)
    inv_rms = lax.rsqrt(jnp.mean(x_float * x_float, axis=-1, keepdims=True) + EPSILON)
    return (x_float * inv_rms * norm_weight.astype(jnp.float32)).astype(jnp.bfloat16)


def route_gates(hidden, expert_ids, router_w, router_b):
    logits = jnp.dot(hidden, router_w, preferred_element_type=jnp.float32) + router_b.astype(jnp.float32)
    chosen = expert_ids[:, :, None] == jnp.arange(logits.shape[1], dtype=jnp.int32)
    return jax.nn.softmax(jnp.sum(jnp.where(chosen, logits[:, None, :], 0.0), axis=-1), axis=-1)


def even_odd(dtype):
    row = lax.broadcasted_iota(jnp.int32, (BLOCK, BLOCK), 0)
    col = lax.broadcasted_iota(jnp.int32, (BLOCK, BLOCK), 1)
    return (row == jnp.where(col < HALF, 2 * col, 2 * (col - HALF) + 1)).astype(jnp.float32).astype(dtype)


def split_kernel(w_ref, low_ref, high_ref):
    perm = even_odd(jnp.bfloat16)
    per_half = low_ref.shape[1] // BLOCK
    for i in range(2 * per_half):
        out = low_ref if i < per_half else high_ref
        part = jnp.dot(w_ref[0, :, i * BLOCK:(i + 1) * BLOCK], perm, preferred_element_type=jnp.float32)
        j = i % per_half
        out[:, j * BLOCK:(j + 1) * BLOCK] = part.astype(jnp.bfloat16)


def split_columns(w):
    _, rows, cols = w.shape
    tile = rows // 4
    return pl.pallas_call(
        split_kernel,
        grid=(4,),
        in_specs=[pl.BlockSpec((1, tile, cols), lambda i: (0, i, 0))],
        out_specs=[pl.BlockSpec((tile, cols // 2), lambda i: (i, 0))] * 2,
        out_shape=[jax.ShapeDtypeStruct((rows, cols // 2), w.dtype)] * 2,
        cost_estimate=pl.CostEstimate(flops=2 * rows * cols * BLOCK, bytes_accessed=4 * rows * cols, transcendentals=0),
        name='split_columns',
    )(w)


def pick_kernel(slot_ref, tok_ref, out_ref):
    experts, sources, capacity, d_model = out_ref.shape
    lanes = lax.broadcasted_iota(jnp.int32, (capacity, tok_ref.shape[1]), 0)
    for s in range(sources):
        picks = jnp.concatenate([(lanes == slot_ref[s, e:e + 1, :]).astype(jnp.float32) for e in range(experts)], axis=0).astype(jnp.bfloat16)
        for n in range(0, d_model, 512):
            rows = jnp.dot(picks, tok_ref[s, :, n:n + 512], preferred_element_type=jnp.float32).astype(jnp.bfloat16)
            for e in range(experts):
                out_ref[e, s, :, n:n + 512] = rows[e * capacity:(e + 1) * capacity]


def pick_rows(slot, tokens, capacity):
    sources, experts, tok_dev = slot.shape
    d_model = tokens.shape[2]
    return pl.pallas_call(
        pick_kernel,
        grid=(sources // GROUP,),
        in_specs=[pl.BlockSpec((GROUP, experts, tok_dev), lambda i: (i, 0, 0)), pl.BlockSpec((GROUP, tok_dev, d_model), lambda i: (i, 0, 0))],
        out_specs=pl.BlockSpec((experts, GROUP, capacity, d_model), lambda i: (0, i, 0, 0)),
        out_shape=jax.ShapeDtypeStruct((experts, sources, capacity, d_model), jnp.bfloat16),
        cost_estimate=pl.CostEstimate(flops=2 * sources * experts * capacity * tok_dev * d_model, bytes_accessed=2 * sources * d_model * (tok_dev + experts * capacity), transcendentals=0),
        name='pick_rows',
    )(slot, tokens)


def gate_up_kernel(x_ref, *refs, jobs):
    w_refs, bias_refs, out_refs = refs[:jobs], refs[jobs:2 * jobs], refs[2 * jobs:]
    steps = pl.num_programs(0) // jobs
    for j in range(jobs):
        @pl.when(pl.program_id(0) // steps == j)
        def _():
            perm = even_odd(jnp.bfloat16)
            bias = jnp.broadcast_to(bias_refs[j][0].astype(jnp.float32), (16, BLOCK)).astype(jnp.bfloat16)
            bias = jnp.dot(bias, perm, preferred_element_type=jnp.float32)[0:1]
            u = jnp.dot(x_ref[0], w_refs[j][...], preferred_element_type=jnp.float32)
            u = (u + bias).astype(jnp.bfloat16).astype(jnp.float32)
            gate = jnp.minimum(u[:, :HALF], LIMIT)
            linear = jnp.clip(u[:, HALF:], -LIMIT, LIMIT)
            out_refs[j][...] = (gate * jax.nn.sigmoid(ALPHA * gate) * (linear + 1.0)).astype(jnp.bfloat16)


def gate_up(rows, jobs):
    total, d_model = rows.shape[1:]
    steps = jobs[0][2].shape[1] // BLOCK

    def block(j, i):
        return jnp.clip(i - j * steps, 0, steps - 1)

    def expert(i):
        return sum(jnp.where(i // steps == j, job[0], 0) for j, job in enumerate(jobs))

    count = len(jobs)
    return pl.pallas_call(
        functools.partial(gate_up_kernel, jobs=count),
        grid=(count * steps,),
        in_specs=[pl.BlockSpec((1, total, d_model), lambda i: (expert(i), 0, 0))]
        + [pl.BlockSpec((d_model, BLOCK), lambda i, j=j: (0, block(j, i))) for j in range(count)]
        + [pl.BlockSpec((1, 1, BLOCK), lambda i, j=j: (jobs[j][0] % 2, 0, jobs[j][1] * steps + block(j, i))) for j in range(count)],
        out_specs=[pl.BlockSpec((total, HALF), lambda i, j=j: (0, block(j, i))) for j in range(count)],
        out_shape=[jax.ShapeDtypeStruct((total, steps * HALF), jnp.bfloat16)] * count,
        cost_estimate=pl.CostEstimate(flops=2 * count * total * jobs[0][2].size, bytes_accessed=2 * count * (jobs[0][2].size + total * d_model), transcendentals=0),
        name='gate_up',
    )(rows, *[job[2] for job in jobs], *[job[3] for job in jobs])


def down_kernel(*refs, jobs):
    ins, out_refs = refs[:4 * jobs], refs[4 * jobs:]
    steps = pl.num_programs(0) // jobs
    for j in range(jobs):
        z0_ref, z1_ref, w_ref, bias_ref = ins[4 * j:4 * j + 4]

        @pl.when(pl.program_id(0) // steps == j)
        def _():
            z = jnp.concatenate([z0_ref[...], z1_ref[...]], axis=1)
            y = jnp.dot(z, w_ref[...], preferred_element_type=jnp.float32)
            out_refs[j][...] = (y + bias_ref[0].astype(jnp.float32)).astype(jnp.bfloat16)


def down(jobs):
    total, half_ff = jobs[0][0].shape
    d_ff, d_model = jobs[0][2].shape
    tile = 512
    steps, first, count = d_model // tile, 2 * d_ff // tile, len(jobs)

    def block(j, i):
        return jnp.clip(i - j * steps, 0, steps - 1)

    in_specs = []
    for j, job in enumerate(jobs):
        which = job[4]
        in_specs += [pl.BlockSpec((total, half_ff), lambda i: (0, 0))] * 2
        in_specs += [pl.BlockSpec((d_ff, tile), lambda i, j=j: (0, block(j, i))), pl.BlockSpec((1, 1, tile), lambda i, j=j, which=which: (which, 0, first + block(j, i)))]
    return pl.pallas_call(
        functools.partial(down_kernel, jobs=count),
        grid=(count * steps,),
        in_specs=in_specs,
        out_specs=[pl.BlockSpec((total, tile), lambda i, j=j: (0, block(j, i))) for j in range(count)],
        out_shape=[jax.ShapeDtypeStruct((total, d_model), jnp.bfloat16)] * count,
        cost_estimate=pl.CostEstimate(flops=2 * count * total * d_ff * d_model, bytes_accessed=2 * count * (d_ff * d_model + total * d_model), transcendentals=0),
        name='down',
    )(*[a for job in jobs for a in job[:4]])


def gate_terms(slot, gate, experts, capacity):
    lanes = lax.broadcasted_iota(jnp.int32, (capacity, slot.shape[1]), 0)
    spread = jnp.concatenate([jnp.where(lanes == slot[e:e + 1, :], gate[e:e + 1, :], 0.0) for e in experts], axis=0).T
    high = spread.astype(jnp.bfloat16)
    rest = spread - high.astype(jnp.float32)
    mid = rest.astype(jnp.bfloat16)
    low = (rest - mid.astype(jnp.float32)).astype(jnp.bfloat16)
    return jnp.concatenate([low, mid, high], axis=1)


def early_kernel(slot_ref, gate_ref, *refs, experts):
    *y_refs, out_ref, y_all = refs
    sources, capacity, d_model = y_refs[0].shape
    tok_dev = slot_ref.shape[2]
    count = len(experts) * capacity
    for s in range(sources):
        for i in range(len(experts)):
            for term in range(3):
                y_all[s, term * count + i * capacity:term * count + (i + 1) * capacity, :] = y_refs[i][s]
        terms = gate_terms(slot_ref[s], gate_ref[s], experts, capacity)
        for n in range(0, d_model, 512):
            out_ref[s * tok_dev:(s + 1) * tok_dev, n:n + 512] = jnp.dot(terms, y_all[s, :, n:n + 512], preferred_element_type=jnp.float32)


def early_sum(slot, gate, ys, experts):
    sources, count, tok_dev = slot.shape
    capacity, d_model = ys[0].shape[0] // sources, ys[0].shape[1]
    return pl.pallas_call(
        functools.partial(early_kernel, experts=experts),
        grid=(sources // GROUP,),
        in_specs=[pl.BlockSpec((GROUP, count, tok_dev), lambda i: (i, 0, 0))] * 2 + [pl.BlockSpec((GROUP, capacity, d_model), lambda i: (i, 0, 0))] * len(ys),
        out_specs=pl.BlockSpec((GROUP * tok_dev, d_model), lambda i: (i, 0)),
        out_shape=jax.ShapeDtypeStruct((sources * tok_dev, d_model), jnp.float32),
        scratch_shapes=[pltpu.VMEM((GROUP, 3 * len(ys) * capacity, d_model), jnp.bfloat16)],
        cost_estimate=pl.CostEstimate(flops=6 * sources * tok_dev * len(ys) * capacity * d_model, bytes_accessed=sources * d_model * (2 * len(ys) * capacity + 4 * tok_dev), transcendentals=0),
        name='early_sum',
    )(slot, gate, *[y.reshape(sources, capacity, d_model) for y in ys])


def late_kernel(slot_ref, gate_ref, za0, za1, zb0, zb1, wa0, wa1, wb0, wb1, bias_a, bias_b, old_ref, out_ref, y_all, w_all, *, experts):
    group, capacity = GROUP, za0.shape[0] // (2 * GROUP)
    tok_dev = slot_ref.shape[2]
    d_model = out_ref.shape[1]
    first = bias_a.shape[2] - d_model
    count = len(experts) * capacity
    part = lax.rem(pl.program_id(0), 2)

    half_ff = wa0.shape[0]

    @pl.when(pl.program_id(0) == 0)
    def _():
        for i, (w0, w1) in enumerate(((wa0, wa1), (wb0, wb1))):
            w_all[i, :half_ff] = w0[...]
            w_all[i, half_ff:] = w1[...]

    @pl.when(part == 0)
    def _():
        for i, (z0, z1, bias) in enumerate(((za0, za1, bias_a), (zb0, zb1, bias_b))):
            z = jnp.concatenate([z0[...], z1[...]], axis=1)
            for n in range(0, d_model, 512):
                y = jnp.dot(z, w_all[i, :, n:n + 512], preferred_element_type=jnp.float32)
                y = (y + bias[0, :, first + n:first + n + 512].astype(jnp.float32)).astype(jnp.bfloat16)
                for s in range(2 * group):
                    for term in range(3):
                        y_all[s, term * count + i * capacity:term * count + (i + 1) * capacity, n:n + 512] = y[s * capacity:(s + 1) * capacity]

    for s in range(group):
        terms = gate_terms(slot_ref[s], gate_ref[s], experts, capacity)
        for n in range(0, d_model, 512):
            rows = pl.ds(s * tok_dev, tok_dev)
            out_ref[rows, n:n + 512] = old_ref[rows, n:n + 512] + jnp.dot(terms, y_all[part * group + s, :, n:n + 512], preferred_element_type=jnp.float32)


def late_sum(slot, gate, zs, weights, biases, experts, old):
    sources, count, tok_dev = slot.shape
    total, half_ff = zs[0].shape
    d_model = old.shape[1]
    capacity = total // sources
    whole = lambda a: pl.BlockSpec(a.shape, lambda i: (0, 0))
    return pl.pallas_call(
        functools.partial(late_kernel, experts=experts),
        grid=(sources // GROUP,),
        in_specs=[pl.BlockSpec((GROUP, count, tok_dev), lambda i: (i, 0, 0))] * 2
        + [pl.BlockSpec((2 * GROUP * capacity, half_ff), lambda i: (i // 2, 0))] * 4
        + [whole(w) for w in weights] + [pl.BlockSpec((1, 1, b.shape[2]), lambda i, which=which: (which, 0, 0)) for which, b in enumerate(biases)]
        + [pl.BlockSpec((GROUP * tok_dev, d_model), lambda i: (i, 0))],
        out_specs=pl.BlockSpec((GROUP * tok_dev, d_model), lambda i: (i, 0)),
        out_shape=jax.ShapeDtypeStruct(old.shape, jnp.float32),
        scratch_shapes=[pltpu.VMEM((2 * GROUP, 3 * len(experts) * capacity, d_model), jnp.bfloat16), pltpu.VMEM((len(experts), 2 * half_ff, d_model), jnp.bfloat16)],
        cost_estimate=pl.CostEstimate(flops=2 * total * 4 * half_ff * d_model + 6 * old.size * len(experts) * capacity, bytes_accessed=8 * old.size, transcendentals=0),
        name='late_sum',
    )(slot, gate, *zs, *weights, *biases, old)


def solution(mesh):
    torus = Mesh(mesh.devices.reshape(4, 4, 4, 2), ALL)
    rows_spec = P(ALL, None)
    plus = [(i, (i + 1) % 4) for i in range(4)]
    minus = [(i, (i + 3) % 4) for i in range(4)]
    swap = [(0, 1), (1, 0)]

    def local_block(x_in, expert_ids, norm_weight, router_w, router_b, w_gate_up, b_gate_up, w_down, b_down):
        tok_dev, d_model = x_in.shape
        top_k = expert_ids.shape[1]
        capacity = CAPACITY_FACTOR * top_k * tok_dev // 128
        d_ff = w_down.shape[1]
        zi, yi, xi, ci = (lax.axis_index(a) for a in ALL)
        first = (zi * 4 + yi) * 8

        gu0, gu1 = split_columns(w_gate_up)
        b_own = jnp.concatenate([b_gate_up, b_down], axis=1)
        own = dict(wd=w_down[0], gu0=gu0, gu1=gu1, b=jnp.stack([b_own, lax.ppermute(b_own, 'c', swap)]))
        left = {k: lax.ppermute(w, 'x', plus) for k, w in own.items()}
        right = {k: lax.ppermute(w, 'x', minus) for k, w in own.items()}
        far = dict(
            gu0=lax.ppermute(left['gu0'], 'x', plus),
            gu1=lax.ppermute(right['gu1'], 'x', minus),
            wd0=lax.ppermute(left['wd'][:d_ff // 2], 'x', plus),
            wd1=lax.ppermute(right['wd'][d_ff // 2:], 'x', minus),
            b=lax.ppermute(left['b'], 'x', plus),
        )
        sets = [(0, own), (3, left), (1, right), (2, far)]

        hidden = rms_norm(x_in, norm_weight)
        tokens = lax.all_gather(hidden, RING, axis=0, tiled=False).reshape(16, tok_dev, d_model)
        gates = route_gates(hidden, expert_ids, router_w, router_b)
        info = lax.all_gather(jnp.concatenate([expert_ids.T.astype(jnp.float32), gates.T], axis=0), RING, axis=0, tiled=False).reshape(16, 2 * top_k, tok_dev)
        ids, gates = info[:, :top_k].astype(jnp.int32), info[:, top_k:]

        experts = first + jnp.stack([((xi + step) % 4) * 2 + (ci if same else 1 - ci) for step, _ in sets for same in (True, False)])
        match = ids[:, None, :, :] == experts[None, :, None, None]
        member = jnp.any(match, axis=2)
        gate = jnp.sum(jnp.where(match, gates[:, None, :, :], 0.0), axis=2)
        before = (jnp.arange(tok_dev)[:, None] < jnp.arange(tok_dev)[None, :]).astype(jnp.bfloat16)
        rank = jnp.einsum('seu,ut->set', member.astype(jnp.bfloat16), before, preferred_element_type=jnp.float32).astype(jnp.int32)
        slot = jnp.where(member, rank, -1)

        rows = pick_rows(slot, tokens, capacity).reshape(8, 16 * capacity, d_model)
        held = []
        for _, weights in sets:
            held += [weights, {k: w if k == 'b' else lax.ppermute(w, 'c', swap) for k, w in weights.items()}]
        z = {}
        for jobs in GATE_JOBS.values():
            done = gate_up(rows, [(e, i, held[e]['gu%d' % i], held[e]['b']) for e, i in jobs])
            z.update(zip(jobs, done))
        ys = {}
        for jobs in DOWN_JOBS.values():
            ys.update(zip(jobs, down([(z[e, 0], z[e, 1], held[e]['wd'], held[e]['b'], e % 2) for e in jobs])))
        ys = [ys[e] for e in range(6)]
        last = [z[e, i] for e in (6, 7) for i in (0, 1)]
        early = early_sum(slot, gate, ys, range(6))
        total = late_sum(slot, gate, last, [held[e]['wd%d' % i] for e in (6, 7) for i in (0, 1)], [held[6]['b'], held[7]['b']], range(6, 8), early)
        mixed = lax.psum_scatter(total, RING, scatter_dimension=0, tiled=True)
        return (x_in.astype(jnp.float32) + mixed).astype(jnp.bfloat16)

    w3, w2 = P(ALL, None, None), P(ALL, None)
    return jax.shard_map(local_block, mesh=torus, in_specs=(rows_spec, rows_spec, P(), P(), P(), w3, w2, w3, w2), out_specs=rows_spec, check_vma=False)
```
